256 devices in a mesh: dp: 32 (over z_lo, x, y), tensor: 8 (over z_hi, core).
Axes of the slice: x: 4, y: 4, z: 8 (z_hi: 4, z_lo: 2; z = z_hi * 2 + z_lo), core: 2. Of those that a mesh axis runs over, the one named last changes fastest.
Arguments:
- hidden: bfloat16 [4096, 8192], P('dp')
- q_weight: float32 [8192, 4096], P(('dp', 'tensor')), may hold values from -0.0625 to 0.0625
- k_weight: float32 [8192, 1024], P(('dp', 'tensor')), may hold values from -0.0625 to 0.0625
- v_weight: float32 [8192, 1024], P(('dp', 'tensor')), may hold values from -0.0625 to 0.0625
- o_weight: float32 [8192, 4096], P(('dp', 'tensor')), may hold values from -0.09375 to 0.09375
- input_gain: float32 [8192], replicated, may hold values from 0.25 to 1.75
- post_gain: float32 [8192], replicated, may hold values from 0.25 to 1.75
- key_cache: bfloat16 [4096, 64, 8, 128], P('dp', None, 'tensor'), may hold values from -1000 to 1000
- value_cache: bfloat16 [4096, 64, 8, 128], P('dp', None, 'tensor'), may hold values from -6 to 6
- lengths: int32 [4096], P('dp'), may hold values from 1 to 64
Outputs:
- new_hidden: bfloat16 [4096, 8192], P('dp')
- normed: bfloat16 [4096, 8192], P('dp')
- fresh_token_keys: bfloat16 [4096, 8, 128], P('dp', 'tensor')
- new_values: bfloat16 [4096, 8, 128], P('dp', 'tensor')
The draws below stay inside these ranges and needn't reach their ends.
All inputs are finite; a program needn't handle non-finite values.
Results may differ from the reference program's by a relative error of at most 0.012.
The reference program's roundings to bfloat16 on the way count: a program that leaves them out, or rounds other values in their place, can miss the bound.
Values may be sent and summed in bfloat16 or wider, within the bound.
A program may use at most 128 MiB of HBM per device.

```python
import math
import jax
import jax.numpy as jnp
from jax import lax

D = 8192
HEADS = 32
KV_HEADS = 8
HEAD_DIM = 128
CACHE = 64
QD = 4096
KD = 1024
GROUP = 4
BATCH = 4096


def draw_hidden(key, part):
    key_base, key_rows, key_column_slice = jax.random.split(key, 3)
    base = jax.random.normal(key_base, (BATCH, D), jnp.float32)
    row_scale = jnp.exp(jax.random.uniform(key_rows, (BATCH, 1), jnp.float32) * math.log(10.0))
    rising = jnp.exp(jnp.arange(D, dtype=jnp.float32)[None, :] / D * math.log(3.0))
    column_scale = jnp.exp(jax.random.uniform(key_column_slice, (1, D), jnp.float32) * math.log(10.0)) * rising
    return (0.03 * base * row_scale * column_scale).astype(jnp.bfloat16)


def draw_key_cache(key, part):
    key_base = jax.random.fold_in(key, 0)
    shape_full = (BATCH, CACHE, KV_HEADS, HEAD_DIM)
    base = jax.random.normal(key_base, shape_full, jnp.float32)
    return base.astype(jnp.bfloat16)


def touch_ends(entries, rng, low, top_value):
    longest = entries.shape.index(max(entries.shape))
    spots = []
    for shift in (0, 1):
        where = [jax.random.randint(jax.random.fold_in(rng, axis), (), 0, length) for axis, length in enumerate(entries.shape)]
        where[longest] = (where[longest] + shift) % entries.shape[longest]
        spots.append(tuple(where))
    return entries.at[spots[0]].set(low).at[spots[1]].set(top_value)


def block_scale(stream_key, shape, shards, least, top_value):
    loudness = 1.0
    for dim, shards_of in shards:
        heights = jax.random.uniform(jax.random.fold_in(jax.random.fold_in(stream_key, 6), dim), (shards_of,), jnp.float32, least / len(shards), top_value / len(shards))
        loudness = loudness * jnp.repeat(jnp.exp(heights), shape[dim] // shards_of).reshape((-1,) + (1,) * (len(shape) - 1 - dim))
    return loudness


def scatter_about(rng, dims, scale, reach, cuts=(), kind=jnp.bfloat16):
    values = jax.random.normal(rng, dims, jnp.float32) * scale
    if len(cuts) > 0:
        values = block_scale(rng, dims, cuts, -0.22, 0.18) * values
    return jnp.clip(values, min=-reach, max=reach).astype(kind)


def setup_inputs(seed: int = 0) -> dict:
    arg_keys = jax.random.split(jax.random.key(seed), 11)
    return {
        "hidden": draw_hidden(jax.random.fold_in(arg_keys[10], 71), 0),
        "q_weight": scatter_about(arg_keys[1], (D, QD), D ** -0.5, 0.0625, ((0, 256),), jnp.float32),
        "k_weight": scatter_about(arg_keys[2], (D, KD), D ** -0.5, 0.0625, ((0, 256),), jnp.float32),
        "v_weight": scatter_about(arg_keys[3], (D, KD), D ** -0.5, 0.0625, ((0, 256),), jnp.float32),
        "o_weight": scatter_about(arg_keys[4], (D, QD), QD ** -0.5, 0.09375, ((0, 256),), jnp.float32),
        "input_gain": jnp.clip(1.0 + 0.15 * jax.random.normal(arg_keys[5], (D,), jnp.float32), 0.25, 1.75),
        "post_gain": jnp.clip(1.0 + 0.15 * jax.random.normal(arg_keys[6], (D,), jnp.float32), 0.25, 1.75),
        "key_cache": draw_key_cache(jax.random.fold_in(arg_keys[10], 71), 0),
        "value_cache": scatter_about(arg_keys[8], (BATCH, CACHE, KV_HEADS, HEAD_DIM), 1.0, 6.0, ((0, 32), (2, 8))),
        "lengths": touch_ends(jax.random.randint(arg_keys[9], (BATCH,), 1, CACHE + 1), jax.random.fold_in(arg_keys[9], 1), 1, CACHE).astype(jnp.int32),
    }


epsilon = 1e-05
rope_base = 500000.0

def rms_gain(values, gain_vector):
    mean_square = lax.optimization_barrier(jnp.mean(values * values, axis=-1, keepdims=True))
    return values * lax.rsqrt(mean_square + epsilon) * gain_vector

def rotate(values, positions):
    half_dim = values.shape[-1] // 2
    index_row = jnp.arange(half_dim, dtype=jnp.float32)
    frequency = jnp.exp(-math.log(rope_base) * index_row / half_dim)
    angle = positions.astype(jnp.float32)[:, None, None] * frequency[None, None, :]
    first_half = values[..., :half_dim]
    second_half = values[..., half_dim:]
    return jnp.concatenate([first_half * jnp.cos(angle) - second_half * jnp.sin(angle), second_half * jnp.cos(angle) + first_half * jnp.sin(angle)], axis=-1)

def reference(hidden, q_weight, k_weight, v_weight, o_weight, input_gain, post_gain, key_cache, value_cache, lengths):
    w_query = q_weight.astype(jnp.bfloat16)
    w_key = k_weight.astype(jnp.bfloat16)
    value_matrix = v_weight.astype(jnp.bfloat16)
    w_out = o_weight.astype(jnp.bfloat16)
    row_count = hidden.shape[0]
    normal_in = rms_gain(hidden.astype(jnp.float32), input_gain).astype(jnp.bfloat16)
    query = jnp.dot(normal_in, w_query, preferred_element_type=jnp.float32)
    key_part = jnp.dot(normal_in, w_key, preferred_element_type=jnp.float32)
    value_part = jnp.dot(normal_in, value_matrix, preferred_element_type=jnp.float32)
    query_b = rotate(query.reshape(row_count, HEADS, HEAD_DIM), lengths).astype(jnp.bfloat16)
    fresh_token_keys = rotate(key_part.reshape(row_count, KV_HEADS, HEAD_DIM), lengths).astype(jnp.bfloat16)
    new_values = value_part.reshape(row_count, KV_HEADS, HEAD_DIM).astype(jnp.bfloat16)
    grouped_heads = query_b.astype(jnp.float32).reshape(row_count, KV_HEADS, GROUP, HEAD_DIM)
    reciprocal_root = 1.0 / math.sqrt(HEAD_DIM)
    scores = jnp.einsum('bkgd,blkd->bkgl', grouped_heads, key_cache.astype(jnp.float32)) * reciprocal_root
    self_token_score = jnp.einsum('lfxa,lfa->lfx', grouped_heads, fresh_token_keys.astype(jnp.float32)) * reciprocal_root
    visible = jnp.arange(CACHE, dtype=jnp.int32)[None, :] < lengths.astype(jnp.int32)[:, None]
    scores = jnp.where(visible[:, None, None, :], scores, -jnp.inf)
    largest = jnp.maximum(lax.optimization_barrier(jnp.max(scores, axis=-1)), self_token_score)
    kept_exp = jnp.exp(scores - largest[..., None])
    own_exp = jnp.exp(self_token_score - largest)
    softmax_divisor = lax.optimization_barrier(jnp.sum(kept_exp, axis=-1)) + own_exp
    weights_kept = (kept_exp / softmax_divisor[..., None]).astype(jnp.bfloat16)
    own_weight = (own_exp / softmax_divisor).astype(jnp.bfloat16)
    attended = jnp.einsum('bkgl,blkd->bkgd', weights_kept.astype(jnp.float32), value_cache.astype(jnp.float32))
    attended = attended + own_weight.astype(jnp.float32)[..., None] * new_values.astype(jnp.float32)[:, :, None, :]
    attended = attended.reshape(row_count, HEADS * HEAD_DIM).astype(jnp.bfloat16)
    mixed = jnp.dot(attended, w_out.T, preferred_element_type=jnp.float32)
    residual = hidden.astype(jnp.float32) + mixed
    new_hidden = residual.astype(jnp.bfloat16)
    normed = rms_gain(residual, post_gain).astype(jnp.bfloat16)
    return (new_hidden, normed, fresh_token_keys, new_values)
```

```python
import math

import jax
import jax.numpy as jnp
from jax import lax
from jax.experimental import pallas as pl
from jax.experimental.pallas import tpu as pltpu
from jax.sharding import PartitionSpec as P

HEAD_DIM = 128
GROUP = 4
ROWS = 128
D = 8192
CACHE = 64
QC = GROUP * HEAD_DIM
WC = QC + 2 * HEAD_DIM
K = 1024
BLOCK_ROWS = 8

epsilon = 1e-05
rope_base = 500000.0

PEERS = [(1, 0), (1, 1), (1, 3), (1, 2), (0, 1), (0, 3), (0, 2)]


def remote(src, dst, send, recv, dp, tensor):
    return pltpu.make_async_remote_copy(
        src_ref=src,
        dst_ref=dst,
        send_sem=send,
        recv_sem=recv,
        device_id={"dp": dp, "tensor": tensor},
        device_id_type=pl.DeviceIdType.MESH,
    )


def kernel(
    hidden_in,
    qw_in,
    kw_in,
    vw_in,
    ow_in,
    gain_in,
    post_in,
    kc_in,
    vc_in,
    cos_in,
    sin_in,
    len_in,
    new_out,
    normed_out,
    fresh_out,
    value_out,
    hidden,
    qw,
    kw,
    vw,
    ow,
    gain,
    post,
    kc,
    vc,
    cos,
    sin,
    lens,
    xn,
    wst,
    ost,
    wg,
    og,
    a,
    pst,
    crecv,
    own,
    probs,
    att32,
    attg,
    half,
    hrecv,
    summed,
    sst,
    srecv,
    tst,
    g,
    gall,
    residual,
    new_v,
    normed_v,
    fresh_v,
    value_v,
    in_sem,
    out_sem,
    b1_s,
    b1_r,
    b2_s,
    b2_r,
    o1_s,
    o1_r,
    o2_s,
    o2_r,
    a_s,
    a_r,
    af_s,
    af_r,
    c_s,
    c_r,
    g_s,
    g_r,
    h_s,
    h_r,
    s_s,
    s_r,
    t_s,
    t_r,
    u_s,
    u_r,
    uf_s,
    uf_r,
):
    dp = lax.axis_index("dp")
    t = lax.axis_index("tensor")
    y = dp % 4
    x = (dp // 4) % 4
    zl = dp // 16
    k = dp // 4
    zh = t // 2
    c = t % 2
    mate = t + 1 - 2 * c

    def member(dz, i):
        return ((zl + dz) % 2) * 4 + (x + i) % 4

    def source(dz, i):
        return ((zl + dz) % 2) * 4 + (x - i + 4) % 4

    def shifted(dz):
        if dz == 0:
            return t
        return ((zh - c * (1 - 2 * zl) + 4) % 4) * 2 + c

    loads = [
        pltpu.make_async_copy(src, dst, in_sem.at[n])
        for n, (src, dst) in enumerate(
            (
                (qw_in, qw),
                (kw_in, kw),
                (vw_in, vw),
                (hidden_in, hidden),
                (gain_in, gain),
                (ow_in, ow),
                (cos_in, cos),
                (sin_in, sin),
                (len_in, lens),
                (kc_in, kc),
                (vc_in, vc),
                (post_in, post),
            )
        )
    ]
    for copy in loads:
        copy.start()

    barrier = pltpu.get_barrier_semaphore()
    greeted = [(member(dz, i) * 4 + y, t) for dz, i in PEERS]
    greeted += [(member(1, i) * 4 + y, shifted(1)) for i in range(4)]
    greeted += [(dp, (t + j) % 8) for j in range(1, 8)]
    greeted += [(k * 4 + (y + i) % 4, t) for i in range(1, 4)]
    for peer in greeted:
        pl.semaphore_signal(
            barrier,
            inc=1,
            device_id={"dp": peer[0], "tensor": peer[1]},
            device_id_type=pl.DeviceIdType.MESH,
        )

    sent = []

    for n in (0, 1, 2):
        loads[n].wait()
    for j in range(8):
        wst[j, :, :QC] = qw[:, j * QC : (j + 1) * QC].astype(jnp.bfloat16)
        wst[j, :, QC : QC + HEAD_DIM] = kw[:, j * HEAD_DIM : (j + 1) * HEAD_DIM].astype(
            jnp.bfloat16
        )
        wst[j, :, QC + HEAD_DIM :] = vw[:, j * HEAD_DIM : (j + 1) * HEAD_DIM].astype(jnp.bfloat16)
    wg[y, t] = wst[t]
    pl.semaphore_wait(barrier, len(greeted))

    order = [4, 2, 6, 3, 5, 1, 7]
    b1 = {}
    for j in order:
        to = (t + j) % 8
        b1[j] = remote(wst.at[to], wg.at[y, t], b1_s.at[j], b1_r.at[j], dp, to)
        b1[j].start()
    sent += b1.values()

    loads[3].wait()
    loads[4].wait()

    def norm_rows(n, carry):
        rows = pl.ds(pl.multiple_of(n * 16, 16), 16)
        values = hidden[rows, :].astype(jnp.float32)
        mean_square = jnp.mean(values * values, axis=-1, keepdims=True)
        normal = (values * lax.rsqrt(mean_square + epsilon) * gain[...]).astype(jnp.bfloat16)
        for m in range(8):
            xn[m, rows, :] = normal[:, m * K : (m + 1) * K]
        return carry

    lax.fori_loop(0, ROWS // 16, norm_rows, 0)

    mine = pl.ds(pl.multiple_of(c * 64, 64), 64)
    ac = {}
    for dz, i in PEERS:
        to = member(dz, i)
        ac[dz, i] = remote(
            xn.at[to, mine],
            a.at[k, mine],
            a_s.at[dz, i],
            a_r.at[dz, i],
            to * 4 + y,
            shifted(dz),
        )
        ac[dz, i].start()
    sent += ac.values()
    a[k] = xn[k]

    loads[5].wait()
    for j in range(8):
        ost[j] = ow[:, j * QC : (j + 1) * QC].astype(jnp.bfloat16)
    og[y, t] = ost[t]
    o1 = {}
    for j in order:
        to = (t + j) % 8
        o1[j] = remote(ost.at[to], og.at[y, t], o1_s.at[j], o1_r.at[j], dp, to)
        o1[j].start()
    sent += o1.values()

    b2 = {}
    for j in [0, 1, 7, 2, 6, 3, 5, 4]:
        if j:
            b1[j].wait_recv()
        origin = (t - j + 8) % 8
        for i in (1, 3, 2):
            b2[j, i] = remote(
                wg.at[y, origin],
                wg.at[y, origin],
                b2_s.at[j, i],
                b2_r.at[j, i],
                k * 4 + (y + i) % 4,
                t,
            )
            b2[j, i].start()
    sent += b2.values()

    af = {}
    for dz, i in [(1, 0), (0, 1), (0, 3), (1, 1), (1, 3), (0, 2), (1, 2)]:
        ac[dz, i].wait_recv()
        at = a.at[source(dz, i), mine]
        af[dz, i] = remote(at, at, af_s.at[dz, i], af_r.at[dz, i], dp, mate)
        af[dz, i].start()
    sent += af.values()

    for copy in b2.values():
        copy.wait_recv()
    for copy in af.values():
        copy.wait_recv()

    weights = wg[...].reshape(K, WC)
    cc = {}
    for dz in (1, 0):
        part = (zl + dz) % 2
        rows = a[pl.ds(part * 4, 4)].reshape(4 * ROWS, K)
        out = jnp.dot(rows, weights, preferred_element_type=jnp.float32).reshape(4, ROWS, WC)
        pst[pl.ds(part * 4, 4)] = out.astype(jnp.bfloat16)
        for i in (1, 3, 2, 0):
            if (dz, i) == (0, 0):
                continue
            to = member(dz, i)
            cc[dz, i] = remote(
                pst.at[to], crecv.at[dz, i], c_s.at[dz, i], c_r.at[dz, i], to * 4 + y, t
            )
            cc[dz, i].start()
    sent += cc.values()

    o2 = {}
    for j in [0, 1, 7, 2, 6, 3, 5, 4]:
        if j:
            o1[j].wait_recv()
        origin = (t - j + 8) % 8
        for i in (1, 3, 2):
            o2[j, i] = remote(
                og.at[y, origin],
                og.at[y, origin],
                o2_s.at[j, i],
                o2_r.at[j, i],
                k * 4 + (y + i) % 4,
                t,
            )
            o2[j, i].start()
    sent += o2.values()

    own[...] = pst[k].astype(jnp.float32)
    for dz, i in [(1, 0), (0, 1), (0, 3), (1, 1), (1, 3), (0, 2), (1, 2)]:
        cc[dz, i].wait_recv()
        own[...] += crecv[dz, i].astype(jnp.float32)

    for n in range(6, 11):
        loads[n].wait()

    cosine = cos[...]
    sine = sin[...]
    for h in range(GROUP + 1):
        columns = slice(h * HEAD_DIM, (h + 1) * HEAD_DIM)
        head = own[:, columns]
        head = head * cosine + pltpu.roll(head, 64, 1) * sine
        own[:, columns] = head.astype(jnp.bfloat16).astype(jnp.float32)
    fresh_v[...] = own[:, QC : QC + HEAD_DIM].astype(jnp.bfloat16)
    value_b = own[:, QC + HEAD_DIM :].astype(jnp.bfloat16)
    value_v[...] = value_b
    own[:, QC + HEAD_DIM :] = value_b.astype(jnp.float32)

    scale = 1.0 / math.sqrt(HEAD_DIM)
    wide = BLOCK_ROWS * CACHE
    tall = BLOCK_ROWS * GROUP
    row_of = lax.broadcasted_iota(jnp.int32, (tall, wide), 0) % BLOCK_ROWS
    column = lax.broadcasted_iota(jnp.int32, (tall, wide), 1)
    same = row_of == column // CACHE
    position = column % CACHE
    for n in range(ROWS // BLOCK_ROWS):
        rows = slice(n * BLOCK_ROWS, (n + 1) * BLOCK_ROWS)
        query = jnp.concatenate(
            [own[rows, h * HEAD_DIM : (h + 1) * HEAD_DIM] for h in range(GROUP)], axis=0
        )
        fresh = jnp.concatenate([own[rows, QC : QC + HEAD_DIM]] * GROUP, axis=0)
        length = jnp.concatenate([lens[rows, :]] * GROUP, axis=0)
        scores = (
            lax.dot_general(
                query.astype(jnp.bfloat16),
                kc[n * wide : (n + 1) * wide, :],
                (((1,), (1,)), ((), ())),
                preferred_element_type=jnp.float32,
            )
            * scale
        )
        self_score = jnp.sum(query * fresh, axis=-1, keepdims=True) * scale
        kept = same & (position < length)
        scores = jnp.where(kept, scores, -jnp.inf)
        largest = jnp.maximum(jnp.max(scores, axis=-1, keepdims=True), self_score)
        kept_exp = jnp.exp(scores - largest)
        own_exp = jnp.exp(self_score - largest)
        divisor = jnp.sum(kept_exp, axis=-1, keepdims=True) + own_exp
        probs[n] = (kept_exp / divisor).astype(jnp.bfloat16)
        own_prob = (own_exp / divisor).astype(jnp.bfloat16).astype(jnp.float32)
        value = jnp.concatenate([own[rows, QC + HEAD_DIM :]] * GROUP, axis=0)
        attended = (
            jnp.dot(
                probs[n],
                vc[n * wide : (n + 1) * wide, :],
                preferred_element_type=jnp.float32,
            )
            + own_prob * value
        )
        for h in range(GROUP):
            att32[rows, h * HEAD_DIM : (h + 1) * HEAD_DIM] = attended[
                h * BLOCK_ROWS : (h + 1) * BLOCK_ROWS
            ]

    attg[k] = att32[...].astype(jnp.bfloat16)
    gc = {}
    for dz, i in PEERS:
        gc[dz, i] = remote(
            attg.at[k], attg.at[k], g_s.at[dz, i], g_r.at[dz, i], member(dz, i) * 4 + y, t
        )
        gc[dz, i].start()
    sent += gc.values()

    for copy in o2.values():
        copy.wait_recv()
    for copy in gc.values():
        copy.wait_recv()

    hc = {}
    theirs_w = og[pl.ds((1 - c) * 2, 2)].reshape(512, QC)
    mine_w = og[pl.ds(c * 2, 2)].reshape(512, QC)
    for n in range(2):
        rows = attg[4 * n : 4 * n + 4].reshape(4 * ROWS, QC)
        half[n] = lax.dot_general(
            rows, theirs_w, (((1,), (1,)), ((), ())), preferred_element_type=jnp.float32
        ).astype(jnp.bfloat16)
        hc[n] = remote(half.at[n], hrecv.at[n], h_s.at[n], h_r.at[n], dp, mate)
        hc[n].start()
    sent += hc.values()
    for n in range(2):
        rows = attg[4 * n : 4 * n + 4].reshape(4 * ROWS, QC)
        summed[n] = lax.dot_general(
            rows, mine_w, (((1,), (1,)), ((), ())), preferred_element_type=jnp.float32
        )
    for n in range(2):
        hc[n].wait_recv()
        both = summed[n] + hrecv[n].astype(jnp.float32)
        for b in range(4):
            sst[b, n * 512 : (n + 1) * 512, :] = both[:, b * 128 : (b + 1) * 128].astype(
                jnp.bfloat16
            )
    sc = {}
    for j in (2, 1, 3):
        to = (zh + j) % 4
        sc[j] = remote(sst.at[to], srecv.at[j], s_s.at[j], s_r.at[j], dp, to * 2 + c)
        sc[j].start()
    sent += sc.values()
    for j in (1, 3, 2):
        sc[j].wait_recv()
    total = (
        sst[zh].astype(jnp.float32)
        + srecv[1].astype(jnp.float32)
        + srecv[2].astype(jnp.float32)
        + srecv[3].astype(jnp.float32)
    )
    tst[...] = total.astype(jnp.bfloat16).reshape(8, ROWS, 128)

    tc = {}
    for dz, i in PEERS:
        to = member(dz, i)
        tc[dz, i] = remote(
            tst.at[to], g.at[k], t_s.at[dz, i], t_r.at[dz, i], to * 4 + y, t
        )
        tc[dz, i].start()
    sent += tc.values()
    g[k] = tst[k]
    for copy in tc.values():
        copy.wait_recv()
    uc = {}
    for j in (2, 1, 3):
        to = (zh + j) % 4
        uc[j] = remote(g, gall.at[zh, c], u_s.at[j], u_r.at[j], dp, to * 2 + c)
        uc[j].start()
    uf = {}
    uf[0] = remote(g, gall.at[zh, c], uf_s.at[0], uf_r.at[0], dp, mate)
    uf[0].start()
    gall[zh, c] = g[...]
    for j in (1, 3, 2):
        uc[j].wait_recv()
        at = gall.at[(zh - j + 4) % 4, c]
        uf[j] = remote(at, at, uf_s.at[j], uf_r.at[j], dp, mate)
        uf[j].start()
    sent += uc.values()
    sent += uf.values()
    for copy in uf.values():
        copy.wait_recv()
    loads[11].wait()

    def finish(n, carry):
        rows = pl.ds(pl.multiple_of(n * 16, 16), 16)
        squares = jnp.zeros((16, 128), jnp.float32)
        for b in range(64):
            columns = slice(b * 128, (b + 1) * 128)
            mixed = gall[b % 4, (b // 4) % 2, b // 8, rows, :].astype(jnp.float32)
            value = hidden[rows, columns].astype(jnp.float32) + mixed
            new_v[rows, columns] = value.astype(jnp.bfloat16)
            residual[:, columns] = value
            squares += value * value
        mean_square = jnp.sum(squares, axis=-1, keepdims=True) * (1.0 / D)
        factor = lax.rsqrt(mean_square + epsilon)
        normed_v[rows, :] = (residual[...] * factor * post[...]).astype(jnp.bfloat16)
        return carry

    lax.fori_loop(0, ROWS // 16, finish, 0)

    stores = [
        pltpu.make_async_copy(src, dst, out_sem.at[n])
        for n, (src, dst) in enumerate(
            ((new_v, new_out), (normed_v, normed_out), (fresh_v, fresh_out), (value_v, value_out))
        )
    ]
    for copy in stores:
        copy.start()
    for copy in stores:
        copy.wait()
    for copy in sent:
        copy.wait_send()


def shards(
    hidden,
    q_weight,
    k_weight,
    v_weight,
    o_weight,
    input_gain,
    post_gain,
    key_cache,
    value_cache,
    lengths,
):
    half_dim = HEAD_DIM // 2
    index_row = jnp.arange(half_dim, dtype=jnp.float32)
    frequency = jnp.exp(-math.log(rope_base) * index_row / half_dim)
    angle = lengths.astype(jnp.float32)[:, None] * frequency[None, :]
    cosine, sine = jnp.cos(angle), jnp.sin(angle)
    cos = jnp.concatenate([cosine, cosine], axis=-1)
    sin = jnp.concatenate([-sine, sine], axis=-1)
    lens = lengths.astype(jnp.int32)[:, None]
    kc = jnp.transpose(key_cache, (0, 2, 1, 3)).reshape(ROWS * CACHE, HEAD_DIM)
    vc = jnp.transpose(value_cache, (0, 2, 1, 3)).reshape(ROWS * CACHE, HEAD_DIM)
    bf16, f32 = jnp.bfloat16, jnp.float32
    dma = pltpu.SemaphoreType.DMA
    new_hidden, normed, fresh, values = pl.pallas_call(
        kernel,
        out_shape=(
            jax.ShapeDtypeStruct((ROWS, D), bf16),
            jax.ShapeDtypeStruct((ROWS, D), bf16),
            jax.ShapeDtypeStruct((ROWS, HEAD_DIM), bf16),
            jax.ShapeDtypeStruct((ROWS, HEAD_DIM), bf16),
        ),
        in_specs=[pl.BlockSpec(memory_space=pl.ANY)] * 12,
        out_specs=[pl.BlockSpec(memory_space=pl.ANY)] * 4,
        scratch_shapes=[
            pltpu.VMEM((ROWS, D), bf16),
            pltpu.VMEM((32, 4096), f32),
            pltpu.VMEM((32, 1024), f32),
            pltpu.VMEM((32, 1024), f32),
            pltpu.VMEM((32, 4096), f32),
            pltpu.VMEM((1, D), f32),
            pltpu.VMEM((1, D), f32),
            pltpu.VMEM((ROWS * CACHE, HEAD_DIM), bf16),
            pltpu.VMEM((ROWS * CACHE, HEAD_DIM), bf16),
            pltpu.VMEM((ROWS, HEAD_DIM), f32),
            pltpu.VMEM((ROWS, HEAD_DIM), f32),
            pltpu.VMEM((ROWS, 1), jnp.int32),
            pltpu.VMEM((8, ROWS, K), bf16),
            pltpu.VMEM((8, 32, WC), bf16),
            pltpu.VMEM((8, 32, QC), bf16),
            pltpu.VMEM((4, 8, 32, WC), bf16),
            pltpu.VMEM((4, 8, 32, QC), bf16),
            pltpu.VMEM((8, ROWS, K), bf16),
            pltpu.VMEM((8, ROWS, WC), bf16),
            pltpu.VMEM((2, 4, ROWS, WC), bf16),
            pltpu.VMEM((ROWS, WC), f32),
            pltpu.VMEM((ROWS // BLOCK_ROWS, BLOCK_ROWS * GROUP, BLOCK_ROWS * CACHE), bf16),
            pltpu.VMEM((ROWS, QC), f32),
            pltpu.VMEM((8, ROWS, QC), bf16),
            pltpu.VMEM((2, 512, 512), bf16),
            pltpu.VMEM((2, 512, 512), bf16),
            pltpu.VMEM((2, 512, 512), f32),
            pltpu.VMEM((4, 1024, 128), bf16),
            pltpu.VMEM((4, 1024, 128), bf16),
            pltpu.VMEM((8, ROWS, 128), bf16),
            pltpu.VMEM((8, ROWS, 128), bf16),
            pltpu.VMEM((4, 2, 8, ROWS, 128), bf16),
            pltpu.VMEM((16, D), f32),
            pltpu.VMEM((ROWS, D), bf16),
            pltpu.VMEM((ROWS, D), bf16),
            pltpu.VMEM((ROWS, HEAD_DIM), bf16),
            pltpu.VMEM((ROWS, HEAD_DIM), bf16),
            dma((12,)),
            dma((4,)),
            dma((8,)),
            dma((8,)),
            dma((8, 4)),
            dma((8, 4)),
            dma((8,)),
            dma((8,)),
            dma((8, 4)),
            dma((8, 4)),
            dma((2, 4)),
            dma((2, 4)),
            dma((2, 4)),
            dma((2, 4)),
            dma((2, 4)),
            dma((2, 4)),
            dma((2, 4)),
            dma((2, 4)),
            dma((2,)),
            dma((2,)),
            dma((4,)),
            dma((4,)),
            dma((2, 4)),
            dma((2, 4)),
            dma((4,)),
            dma((4,)),
            dma((4,)),
            dma((4,)),
        ],
        compiler_params=pltpu.CompilerParams(collective_id=0, has_side_effects=True),
    )(
        hidden,
        q_weight,
        k_weight,
        v_weight,
        o_weight,
        input_gain.reshape(1, D),
        post_gain.reshape(1, D),
        kc,
        vc,
        cos,
        sin,
        lens,
    )
    return (
        new_hidden,
        normed,
        fresh.reshape(ROWS, 1, HEAD_DIM),
        values.reshape(ROWS, 1, HEAD_DIM),
    )


def solution(mesh):
    in_specs = (
        P("dp", None),
        P(("dp", "tensor"), None),
        P(("dp", "tensor"), None),
        P(("dp", "tensor"), None),
        P(("dp", "tensor"), None),
        P(),
        P(),
        P("dp", None, "tensor", None),
        P("dp", None, "tensor", None),
        P("dp"),
    )
    out_specs = (P("dp", None), P("dp", None), P("dp", "tensor", None), P("dp", "tensor", None))
    return jax.shard_map(shards, mesh=mesh, in_specs=in_specs, out_specs=out_specs, check_vma=False)
```

```python
import math

import jax
import jax.numpy as jnp
from jax import lax
from jax.experimental import pallas as pl
from jax.experimental.pallas import tpu as pltpu
from jax.sharding import PartitionSpec as P

HEAD_DIM = 128
GROUP = 4
ROWS = 128
D = 8192
CACHE = 64
QD = 4096
QC = GROUP * HEAD_DIM
WC = QC + 2 * HEAD_DIM
K = 1024
BLOCK_ROWS = 8
CHUNKS = 2
CR = ROWS // CHUNKS
CH = CR // 2
FEATURES = 256
FLIGHTS = 160

epsilon = 1e-05
rope_base = 500000.0

PEERS = [(1, 0), (1, 1), (1, 3), (1, 2), (0, 1), (0, 3), (0, 2)]


def kernel(
    hidden_in,
    qw_in,
    kw_in,
    vw_in,
    ow_in,
    gain_in,
    kc_in,
    vc_in,
    len_in,
    mixed_out,
    fresh_out,
    value_out,
    hidden,
    qw,
    kw,
    vw,
    ow,
    gain,
    kc,
    vc,
    len_row,
    lens,
    cos,
    sin,
    xn,
    wst,
    wg,
    og,
    a,
    pst,
    cx,
    cn,
    cf,
    zst,
    zrecv,
    own,
    probs,
    att32,
    attg,
    made,
    gall,
    fresh_v,
    value_v,
    in_sem,
    out_sem,
    send_sem,
    recv_sem,
):
    dp = lax.axis_index("dp")
    t = lax.axis_index("tensor")
    y = dp % 4
    x = (dp // 4) % 4
    zl = dp // 16
    k = dp // 4
    zh = t // 2
    c = t % 2
    mate = t + 1 - 2 * c

    def member(dz, i):
        return ((zl + dz) % 2) * 4 + (x + i) % 4

    def source(dz, i):
        return ((zl + dz) % 2) * 4 + (x - i + 4) % 4

    def shifted(dz):
        if dz == 0:
            return t
        return ((zh - c * (1 - 2 * zl) + 4) % 4) * 2 + c

    def along_x(i):
        return (zl * 4 + (x + i) % 4) * 4 + y

    def along_y(i):
        return k * 4 + (y + i) % 4

    def along_z(j):
        return ((zh + j) % 4) * 2 + c

    across = ((1 - zl) * 4 + x) * 4 + y

    sent = []

    def send(src, dst, to_dp, to_tensor):
        n = len(sent)
        copy = pltpu.make_async_remote_copy(
            src_ref=src,
            dst_ref=dst,
            send_sem=send_sem.at[n],
            recv_sem=recv_sem.at[n],
            device_id={"dp": to_dp, "tensor": to_tensor},
            device_id_type=pl.DeviceIdType.MESH,
        )
        copy.start()
        sent.append(copy)
        return copy

    loads = [
        pltpu.make_async_copy(src, dst, in_sem.at[n])
        for n, (src, dst) in enumerate(
            (
                (qw_in, qw),
                (kw_in, kw),
                (vw_in, vw),
                (hidden_in, hidden),
                (gain_in, gain),
                (len_in, len_row),
                (ow_in, ow),
                (kc_in, kc),
                (vc_in, vc),
            )
        )
    ]
    for copy in loads:
        copy.start()

    barrier = pltpu.get_barrier_semaphore()
    greeted = [(along_x(i), t) for i in range(1, 4)]
    greeted += [(across, t)]
    greeted += [(member(1, i) * 4 + y, shifted(1)) for i in range(4)]
    greeted += [(dp, (t + j) % 8) for j in range(1, 8)]
    greeted += [(along_y(i), t) for i in range(1, 4)]
    for peer in greeted:
        pl.semaphore_signal(
            barrier,
            inc=1,
            device_id={"dp": peer[0], "tensor": peer[1]},
            device_id_type=pl.DeviceIdType.MESH,
        )

    for n in (0, 1, 2):
        loads[n].wait()
    for j in range(8):
        wst[j, :, :QC] = qw[:, j * QC : (j + 1) * QC].astype(jnp.bfloat16)
        wst[j, :, QC : QC + HEAD_DIM] = kw[:, j * HEAD_DIM : (j + 1) * HEAD_DIM].astype(
            jnp.bfloat16
        )
        wst[j, :, QC + HEAD_DIM :] = vw[:, j * HEAD_DIM : (j + 1) * HEAD_DIM].astype(jnp.bfloat16)
    wg[y, t] = wst[t]
    pl.semaphore_wait(barrier, len(greeted))

    b1 = {}
    for j in (4, 2, 6, 3, 5, 1, 7):
        to = (t + j) % 8
        b1[j] = send(wst.at[to], wg.at[y, t], dp, to)

    loads[3].wait()
    loads[4].wait()

    def norm_rows(n, carry):
        rows = pl.ds(pl.multiple_of(n * 16, 16), 16)
        values = hidden[rows, :].astype(jnp.float32)
        mean_square = jnp.mean(values * values, axis=-1, keepdims=True)
        normal = (values * lax.rsqrt(mean_square + epsilon) * gain[...]).astype(jnp.bfloat16)
        for m in range(8):
            xn[m, rows, :] = normal[:, m * K : (m + 1) * K]
        return carry

    lax.fori_loop(0, ROWS // 16, norm_rows, 0)

    mine = pl.ds(pl.multiple_of(c * 64, 64), 64)
    ac = {}
    for dz, i in PEERS:
        to = member(dz, i)
        ac[dz, i] = send(xn.at[to, mine], a.at[k, mine], to * 4 + y, shifted(dz))
    a[k] = xn[k]

    b2 = {}
    arrival = [0, 1, 7, 2, 6, 3, 5, 4]
    for j in arrival:
        if j:
            b1[j].wait_recv()
        at = wg.at[y, (t - j + 8) % 8]
        b2[j, 1] = send(at, at, along_y(1), t)
        b2[j, 3] = send(at, at, along_y(3), t)
    b3 = []
    for j in arrival:
        i = 1 + 2 * (j % 2)
        b2[j, i].wait_recv()
        at = wg.at[(y + 4 - i) % 4, (t - j + 8) % 8]
        b3.append(send(at, at, along_y(i), t))

    loads[5].wait()
    diagonal = lax.broadcasted_iota(jnp.int32, (ROWS, ROWS), 0) == lax.broadcasted_iota(
        jnp.int32, (ROWS, ROWS), 1
    )
    lengths = jnp.sum(
        jnp.where(diagonal, len_row[...].astype(jnp.float32), 0.0), axis=-1, keepdims=True
    )
    lens[...] = lengths
    lane = lax.broadcasted_iota(jnp.int32, (1, HEAD_DIM), 1)
    index_row = (lane % 64).astype(jnp.float32)
    frequency = jnp.exp(-math.log(rope_base) * index_row / 64)
    angle = lengths * frequency
    cos[...] = jnp.cos(angle)
    sin[...] = jnp.where(lane < 64, -1.0, 1.0) * jnp.sin(angle)

    af = []
    for dz, i in [(1, 0), (0, 1), (0, 3), (1, 1), (1, 3), (0, 2), (1, 2)]:
        ac[dz, i].wait_recv()
        at = a.at[source(dz, i), mine]
        af.append(send(at, at, dp, mate))

    for j in arrival:
        b2[j, 3 - 2 * (j % 2)].wait_recv()
    for copy in b3:
        copy.wait_recv()
    for copy in af:
        copy.wait_recv()

    weights = wg[...].reshape(K, WC)
    first, second = slice(0, 64), slice(64, 128)
    near = {}
    far = {}
    for dz in (1, 0):
        part = (zl + dz) % 2
        rows = a[pl.ds(part * 4, 4)].reshape(4 * ROWS, K)
        out = jnp.dot(rows, weights, preferred_element_type=jnp.float32).reshape(4, ROWS, WC)
        pst[dz] = out.astype(jnp.bfloat16)
        far[dz, 0] = send(pst.at[dz, (x + 2) % 4, first], cx.at[dz, 0], along_x(1), t)
        far[dz, 1] = send(pst.at[dz, (x + 2) % 4, second], cx.at[dz, 1], along_x(3), t)
        near[dz, 0, 1] = send(pst.at[dz, (x + 1) % 4, second], cn.at[dz, 0, 1], along_x(1), t)
        near[dz, 1, 0] = send(pst.at[dz, (x + 3) % 4, first], cn.at[dz, 1, 0], along_x(3), t)

    loads[6].wait()
    og[zl, y] = ow[...].astype(jnp.bfloat16)
    at = og.at[zl, y]
    o1 = send(at, at, across, t)
    o2 = [send(at, at, along_y(i), t) for i in (2, 1, 3)]

    for dz in (1, 0):
        far[dz, 0].wait_recv()
        cf[dz, 0] = (
            cx[dz, 0].astype(jnp.float32) + pst[dz, (x + 1) % 4, first].astype(jnp.float32)
        ).astype(jnp.bfloat16)
        near[dz, 0, 0] = send(cf.at[dz, 0], cn.at[dz, 0, 0], along_x(1), t)
        far[dz, 1].wait_recv()
        cf[dz, 1] = (
            cx[dz, 1].astype(jnp.float32) + pst[dz, (x + 3) % 4, second].astype(jnp.float32)
        ).astype(jnp.bfloat16)
        near[dz, 1, 1] = send(cf.at[dz, 1], cn.at[dz, 1, 1], along_x(3), t)

    o1.wait_recv()
    at = og.at[1 - zl, y]
    o2 += [send(at, at, along_y(i), t) for i in (2, 1, 3)]

    zc = []
    for h, rows in enumerate((first, second)):
        near[1, 0, h].wait_recv()
        near[1, 1, h].wait_recv()
        zst[rows, :] = (
            pst[1, x, rows].astype(jnp.float32)
            + cn[1, 0, h].astype(jnp.float32)
            + cn[1, 1, h].astype(jnp.float32)
        ).astype(jnp.bfloat16)
        zc.append(send(zst.at[rows], zrecv.at[rows], across, t))

    loads[7].wait()
    loads[8].wait()
    scale = 1.0 / math.sqrt(HEAD_DIM)
    wide = BLOCK_ROWS * CACHE
    tall = BLOCK_ROWS * GROUP
    row_of = lax.broadcasted_iota(jnp.int32, (tall, wide), 0) % BLOCK_ROWS
    column = lax.broadcasted_iota(jnp.int32, (tall, wide), 1)
    same = row_of == column // CACHE
    position = (column % CACHE).astype(jnp.float32)

    def attend(h):
        chunk = slice(h * CR, (h + 1) * CR)
        cosine = cos[chunk, :]
        sine = sin[chunk, :]
        for m in range(GROUP + 1):
            columns = slice(m * HEAD_DIM, (m + 1) * HEAD_DIM)
            head = own[chunk, columns]
            head = head * cosine + pltpu.roll(head, 64, 1) * sine
            own[chunk, columns] = head.astype(jnp.bfloat16).astype(jnp.float32)
        fresh_v[chunk, :] = own[chunk, QC : QC + HEAD_DIM].astype(jnp.bfloat16)
        value_b = own[chunk, QC + HEAD_DIM :].astype(jnp.bfloat16)
        value_v[chunk, :] = value_b
        own[chunk, QC + HEAD_DIM :] = value_b.astype(jnp.float32)
        for n in range(h * CR // BLOCK_ROWS, (h + 1) * CR // BLOCK_ROWS):
            rows = slice(n * BLOCK_ROWS, (n + 1) * BLOCK_ROWS)
            query = jnp.concatenate(
                [own[rows, m * HEAD_DIM : (m + 1) * HEAD_DIM] for m in range(GROUP)], axis=0
            )
            fresh = jnp.concatenate([own[rows, QC : QC + HEAD_DIM]] * GROUP, axis=0)
            length = jnp.concatenate([lens[rows, :]] * GROUP, axis=0)
            scores = (
                lax.dot_general(
                    query.astype(jnp.bfloat16),
                    kc[n * wide : (n + 1) * wide, :],
                    (((1,), (1,)), ((), ())),
                    preferred_element_type=jnp.float32,
                )
                * scale
            )
            self_score = jnp.sum(query * fresh, axis=-1, keepdims=True) * scale
            kept = same & (position < length)
            scores = jnp.where(kept, scores, -jnp.inf)
            largest = jnp.maximum(jnp.max(scores, axis=-1, keepdims=True), self_score)
            kept_exp = jnp.exp(scores - largest)
            own_exp = jnp.exp(self_score - largest)
            divisor = jnp.sum(kept_exp, axis=-1, keepdims=True) + own_exp
            probs[n] = (kept_exp / divisor).astype(jnp.bfloat16)
            own_prob = (own_exp / divisor).astype(jnp.bfloat16).astype(jnp.float32)
            value = jnp.concatenate([own[rows, QC + HEAD_DIM :]] * GROUP, axis=0)
            attended = (
                jnp.dot(
                    probs[n],
                    vc[n * wide : (n + 1) * wide, :],
                    preferred_element_type=jnp.float32,
                )
                + own_prob * value
            )
            for m in range(GROUP):
                att32[rows, m * HEAD_DIM : (m + 1) * HEAD_DIM] = attended[
                    m * BLOCK_ROWS : (m + 1) * BLOCK_ROWS
                ]

    def tq(d):
        return ((zh + d) % 4) * 2 + c

    def xq(i):
        return (x + i) % 4

    lower, upper = slice(0, CH), slice(CH, CR)
    z1, z2, x1, x2 = {}, {}, {}, {}
    to_mate = {n: [] for n in range(CHUNKS)}

    def hand(n, at):
        to_mate[n].append(send(at, at, dp, mate))

    def spread_x(n, d):
        at = attg.at[n, tq(d), x]
        x1[n, d, 1] = send(at, at, along_x(1), t)
        x1[n, d, 3] = send(at, at, along_x(3), t)
        hand(n, at)

    def z_first(n):
        z1[n, 1].wait_recv()
        at = attg.at[n, tq(3), x, lower]
        z2[n, 1] = send(at, at, dp, along_z(1))
        z1[n, 3].wait_recv()
        at = attg.at[n, tq(1), x, upper]
        z2[n, 3] = send(at, at, dp, along_z(3))
        spread_x(n, 3)
        spread_x(n, 1)

    def z_second(n):
        z2[n, 1].wait_recv()
        z2[n, 3].wait_recv()
        spread_x(n, 2)

    def x_first(n):
        for d in (0, 3, 1, 2):
            x1[n, d, 1].wait_recv()
            at = attg.at[n, tq(d), xq(3)]
            x2[n, d, 1] = send(at.at[lower], at.at[lower], along_x(1), t)
            hand(n, at)
            x1[n, d, 3].wait_recv()
            at = attg.at[n, tq(d), xq(1)]
            x2[n, d, 3] = send(at.at[upper], at.at[upper], along_x(3), t)
            hand(n, at)

    def x_second(n):
        for d in (0, 3, 1, 2):
            x2[n, d, 1].wait_recv()
            x2[n, d, 3].wait_recv()
            hand(n, attg.at[n, tq(d), xq(2)])

    for h, rows in enumerate((first, second)):
        near[0, 0, h].wait_recv()
        near[0, 1, h].wait_recv()
        own[rows, :] = (
            pst[0, x, rows].astype(jnp.float32)
            + cn[0, 0, h].astype(jnp.float32)
            + cn[0, 1, h].astype(jnp.float32)
        )
        zc[h].wait_recv()
        own[rows, :] += zrecv[rows, :].astype(jnp.float32)
        attend(h)
        attg[h, t, x] = att32[rows, :].astype(jnp.bfloat16)
        at = attg.at[h, t, x]
        z1[h, 1] = send(at, at, dp, along_z(1))
        z1[h, 3] = send(at, at, dp, along_z(3))
        spread_x(h, 0)

    z_first(0)
    z_first(1)
    z_second(0)
    z_second(1)

    tc, u1, u2 = {}, {}, {}
    final = {n: [] for n in range(CHUNKS)}

    def project(n):
        for copy in to_mate[n]:
            copy.wait_recv()
        out = jnp.zeros((4 * CR, FEATURES), jnp.float32)
        for j in range(8):
            out += lax.dot_general(
                attg[n, j].reshape(4 * CR, QC),
                og[:, :, :, j * QC : (j + 1) * QC].reshape(FEATURES, QC),
                (((1,), (1,)), ((), ())),
                preferred_element_type=jnp.float32,
            )
        made[n] = out.astype(jnp.bfloat16).reshape(4, CR, FEATURES)
        for i in (2, 1, 3):
            tc[n, i] = send(made.at[n, xq(i)], gall.at[n, t, x], along_x(i), t)
        gall[n, t, x] = made[n, x]

    def gather_first(n):
        for i in (1, 3, 2):
            tc[n, i].wait_recv()
        at = gall.at[n, t]
        u1[n, 1] = send(at, at, dp, along_z(1))
        u1[n, 3] = send(at, at, dp, along_z(3))
        final[n].append(send(at, at, dp, mate))

    def gather_second(n):
        u1[n, 1].wait_recv()
        at = gall.at[n, tq(3)]
        part = at.at[pl.ds(0, 2)]
        u2[n, 1] = send(part, part, dp, along_z(1))
        final[n].append(send(at, at, dp, mate))
        u1[n, 3].wait_recv()
        at = gall.at[n, tq(1)]
        part = at.at[pl.ds(2, 2)]
        u2[n, 3] = send(part, part, dp, along_z(3))
        final[n].append(send(at, at, dp, mate))

    def gather_third(n):
        u2[n, 1].wait_recv()
        u2[n, 3].wait_recv()
        at = gall.at[n, tq(2)]
        final[n].append(send(at, at, dp, mate))

    x_first(0)
    x_second(0)
    for copy in o2:
        copy.wait_recv()
    project(0)
    x_first(1)
    gather_first(0)
    x_second(1)
    project(1)
    gather_second(0)
    gather_first(1)
    gather_third(0)
    gather_second(1)
    stores = [
        pltpu.make_async_copy(src, dst, out_sem.at[n])
        for n, (src, dst) in enumerate(
            (
                (gall.at[0], mixed_out.at[0]),
                (gall.at[1], mixed_out.at[1]),
                (fresh_v, fresh_out),
                (value_v, value_out),
            )
        )
    ]
    stores[2].start()
    stores[3].start()
    for copy in final[0]:
        copy.wait_recv()
    stores[0].start()
    gather_third(1)
    for copy in final[1]:
        copy.wait_recv()
    stores[1].start()
    for copy in stores:
        copy.wait()
    for copy in sent:
        copy.wait_send()


def finish(hidden, mixed, fresh, value, post, new_hidden, normed, fresh_out, value_out, residual):
    lane = lax.broadcasted_iota(jnp.int32, (1, 128), 1)
    squares = jnp.zeros((16, 128), jnp.float32)
    for x in range(4):
        for q in range(2):
            for zl in range(2):
                pieces = [
                    mixed[0, 4 * q + s, x, :, zl * 128 : (zl + 1) * 128].astype(jnp.float32)
                    for s in range(4)
                ]
                turned = [pieces[0]] + [pltpu.roll(pieces[s], 32 * s, 1) for s in range(1, 4)]
                for y in range(4):
                    block = turned[(0 - y) % 4]
                    for p in range(1, 4):
                        block = jnp.where(lane // 32 == p, turned[(p - y) % 4], block)
                    if y:
                        block = pltpu.roll(block, 128 - 32 * y, 1)
                    at = (zl * 16 + x * 4 + y) * 256 + q * 128
                    columns = slice(at, at + 128)
                    total = hidden[:, columns].astype(jnp.float32) + block
                    new_hidden[:, columns] = total.astype(jnp.bfloat16)
                    residual[:, columns] = total
                    squares += total * total
    mean_square = jnp.sum(squares, axis=-1, keepdims=True) * (1.0 / D)
    normed[...] = (residual[...] * lax.rsqrt(mean_square + epsilon) * post[...]).astype(
        jnp.bfloat16
    )
    fresh_out[...] = fresh[...]
    value_out[...] = value[...]


def shards(
    hidden,
    q_weight,
    k_weight,
    v_weight,
    o_weight,
    input_gain,
    post_gain,
    key_cache,
    value_cache,
    lengths,
):
    kc = jnp.transpose(key_cache, (0, 2, 1, 3)).reshape(ROWS * CACHE, HEAD_DIM)
    vc = jnp.transpose(value_cache, (0, 2, 1, 3)).reshape(ROWS * CACHE, HEAD_DIM)
    bf16, f32 = jnp.bfloat16, jnp.float32
    dma = pltpu.SemaphoreType.DMA
    mixed, fresh, values = pl.pallas_call(
        kernel,
        out_shape=(
            jax.ShapeDtypeStruct((CHUNKS, 8, 4, CR, FEATURES), bf16),
            jax.ShapeDtypeStruct((ROWS, HEAD_DIM), bf16),
            jax.ShapeDtypeStruct((ROWS, HEAD_DIM), bf16),
        ),
        in_specs=[pl.BlockSpec(memory_space=pl.ANY)] * 9,
        out_specs=[pl.BlockSpec(memory_space=pl.ANY)] * 3,
        scratch_shapes=[
            pltpu.VMEM((ROWS, D), bf16),
            pltpu.VMEM((32, QD), f32),
            pltpu.VMEM((32, 1024), f32),
            pltpu.VMEM((32, 1024), f32),
            pltpu.VMEM((32, QD), f32),
            pltpu.VMEM((1, D), f32),
            pltpu.VMEM((ROWS * CACHE, HEAD_DIM), bf16),
            pltpu.VMEM((ROWS * CACHE, HEAD_DIM), bf16),
            pltpu.VMEM((1, ROWS), jnp.int32),
            pltpu.VMEM((ROWS, 1), f32),
            pltpu.VMEM((ROWS, HEAD_DIM), f32),
            pltpu.VMEM((ROWS, HEAD_DIM), f32),
            pltpu.VMEM((8, ROWS, K), bf16),
            pltpu.VMEM((8, 32, WC), bf16),
            pltpu.VMEM((4, 8, 32, WC), bf16),
            pltpu.VMEM((2, 4, 32, QD), bf16),
            pltpu.VMEM((8, ROWS, K), bf16),
            pltpu.VMEM((2, 4, ROWS, WC), bf16),
            pltpu.VMEM((2, 2, 64, WC), bf16),
            pltpu.VMEM((2, 2, 2, 64, WC), bf16),
            pltpu.VMEM((2, 2, 64, WC), bf16),
            pltpu.VMEM((ROWS, WC), bf16),
            pltpu.VMEM((ROWS, WC), bf16),
            pltpu.VMEM((ROWS, WC), f32),
            pltpu.VMEM((ROWS // BLOCK_ROWS, BLOCK_ROWS * GROUP, BLOCK_ROWS * CACHE), bf16),
            pltpu.VMEM((ROWS, QC), f32),
            pltpu.VMEM((CHUNKS, 8, 4, CR, QC), bf16),
            pltpu.VMEM((CHUNKS, 4, CR, FEATURES), bf16),
            pltpu.VMEM((CHUNKS, 8, 4, CR, FEATURES), bf16),
            pltpu.VMEM((ROWS, HEAD_DIM), bf16),
            pltpu.VMEM((ROWS, HEAD_DIM), bf16),
            dma((9,)),
            dma((4,)),
            dma((FLIGHTS,)),
            dma((FLIGHTS,)),
        ],
        compiler_params=pltpu.CompilerParams(collective_id=0, has_side_effects=True),
    )(
        hidden,
        q_weight,
        k_weight,
        v_weight,
        o_weight,
        input_gain.reshape(1, D),
        kc,
        vc,
        lengths.reshape(1, ROWS),
    )
    blocks = CR // 16
    wide = pl.BlockSpec((16, D), lambda n: (n, 0))
    narrow = pl.BlockSpec((16, HEAD_DIM), lambda n: (n, 0))
    new_hidden, normed, fresh, values = pl.pallas_call(
        finish,
        grid=(ROWS // 16,),
        out_shape=(
            jax.ShapeDtypeStruct((ROWS, D), bf16),
            jax.ShapeDtypeStruct((ROWS, D), bf16),
            jax.ShapeDtypeStruct((ROWS, HEAD_DIM), bf16),
            jax.ShapeDtypeStruct((ROWS, HEAD_DIM), bf16),
        ),
        in_specs=[
            wide,
            pl.BlockSpec((1, 8, 4, 16, FEATURES), lambda n: (n // blocks, 0, 0, n % blocks, 0)),
            narrow,
            narrow,
            pl.BlockSpec((1, D), lambda n: (0, 0)),
        ],
        out_specs=[wide, wide, narrow, narrow],
        scratch_shapes=[pltpu.VMEM((16, D), f32)],
    )(hidden, mixed, fresh, values, post_gain.reshape(1, D))
    return (
        new_hidden,
        normed,
        fresh.reshape(ROWS, 1, HEAD_DIM),
        values.reshape(ROWS, 1, HEAD_DIM),
    )


def solution(mesh):
    in_specs = (
        P("dp", None),
        P(("dp", "tensor"), None),
        P(("dp", "tensor"), None),
        P(("dp", "tensor"), None),
        P(("dp", "tensor"), None),
        P(),
        P(),
        P("dp", None, "tensor", None),
        P("dp", None, "tensor", None),
        P("dp"),
    )
    out_specs = (P("dp", None), P("dp", None), P("dp", "tensor", None), P("dp", "tensor", None))
    return jax.shard_map(shards, mesh=mesh, in_specs=in_specs, out_specs=out_specs, check_vma=False)
```

```python
import math

import jax
import jax.numpy as jnp
from jax import lax
from jax.experimental import pallas as pl
from jax.experimental.pallas import tpu as pltpu
from jax.sharding import PartitionSpec as P

HEAD_DIM = 128
GROUP = 4
ROWS = 128
D = 8192
CACHE = 64
QD = 4096
QC = GROUP * HEAD_DIM
WC = QC + 2 * HEAD_DIM
K = 1024
BLOCK_ROWS = 8
CHUNKS = 4
CR = ROWS // CHUNKS
CH = CR // 2
HALF = ROWS // 2
QUARTER = ROWS // 4
FEATURES = 256
SENDS = 32
RECEIVES = 128

epsilon = 1e-05
rope_base = 500000.0

PEERS = [(1, 0), (1, 1), (1, 3), (1, 2), (0, 1), (0, 3), (0, 2)]


def kernel(
    hidden_in,
    qw_in,
    kw_in,
    vw_in,
    ow_in,
    gain_in,
    post_in,
    kc_in,
    vc_in,
    len_in,
    new_out,
    normed_out,
    fresh_out,
    value_out,
    hidden,
    qw,
    kw,
    vw,
    ow,
    gain,
    post,
    kc,
    vc,
    len_row,
    lens,
    cos,
    sin,
    xn,
    wst,
    wg,
    og,
    a,
    acc,
    pst,
    cx,
    cn,
    cf,
    zst,
    zrecv,
    own,
    probs,
    att32,
    attg,
    made,
    gall,
    turn,
    runs,
    ordered,
    residual,
    new_v,
    normed_v,
    fresh_v,
    value_v,
    in_sem,
    out_sem,
    send_sem,
    recv_sem,
):
    dp = lax.axis_index("dp")
    t = lax.axis_index("tensor")
    y = dp % 4
    x = (dp // 4) % 4
    zl = dp // 16
    k = dp // 4
    zh = t // 2
    c = t % 2
    mate = t + 1 - 2 * c

    def member(dz, i):
        return ((zl + dz) % 2) * 4 + (x + i) % 4

    def source(dz, i):
        return ((zl + dz) % 2) * 4 + (x - i + 4) % 4

    def shifted(dz):
        if dz == 0:
            return t
        return ((zh - c * (1 - 2 * zl) + 4) % 4) * 2 + c

    def along_x(i):
        return (zl * 4 + (x + i) % 4) * 4 + y

    def along_y(i):
        return k * 4 + (y + i) % 4

    def along_z(j):
        return ((zh + j) % 4) * 2 + c

    across = ((1 - zl) * 4 + x) * 4 + y

    out_groups, in_groups, out_size, in_size = {}, {}, {}, {}

    def describe(src, dst, out_key, in_key, to_dp, to_tensor):
        n = out_groups.setdefault(out_key, len(out_groups))
        m = in_groups.setdefault(in_key, len(in_groups))
        assert n < SENDS and m < RECEIVES
        return pltpu.make_async_remote_copy(
            src_ref=src,
            dst_ref=dst,
            send_sem=send_sem.at[n],
            recv_sem=recv_sem.at[m],
            device_id={"dp": to_dp, "tensor": to_tensor},
            device_id_type=pl.DeviceIdType.MESH,
        )

    def send(src, dst, out_key, in_key, to_dp, to_tensor):
        size = math.prod(src.shape)
        assert size == math.prod(dst.shape)
        out_size[out_key] = out_size.get(out_key, 0) + size
        in_size[in_key] = in_size.get(in_key, 0) + size
        describe(src, dst, out_key, in_key, to_dp, to_tensor).start()

    def received(in_key, ref):
        assert in_size.pop(in_key) == math.prod(ref.shape)
        describe(ref, ref, next(iter(out_groups)), in_key, dp, mate).wait_recv()

    def departed(out_key, ref):
        assert out_size.pop(out_key) == math.prod(ref.shape)
        describe(ref, ref, out_key, next(iter(in_groups)), dp, mate).wait_send()

    loads = [
        pltpu.make_async_copy(src, dst, in_sem.at[n])
        for n, (src, dst) in enumerate(
            (
                (qw_in, qw),
                (kw_in, kw),
                (vw_in, vw),
                (hidden_in, hidden),
                (gain_in, gain),
                (len_in, len_row),
                (ow_in, ow),
                (kc_in, kc),
                (vc_in, vc),
                (post_in, post),
            )
        )
    ]
    for copy in loads:
        copy.start()

    barrier = pltpu.get_barrier_semaphore()
    greeted = [(along_x(i), t) for i in range(1, 4)]
    greeted += [(across, t)]
    greeted += [(member(1, i) * 4 + y, shifted(1)) for i in range(4)]
    greeted += [(dp, (t + j) % 8) for j in range(1, 8)]
    greeted += [(along_y(i), t) for i in range(1, 4)]
    for peer in greeted:
        pl.semaphore_signal(
            barrier,
            inc=1,
            device_id={"dp": peer[0], "tensor": peer[1]},
            device_id_type=pl.DeviceIdType.MESH,
        )

    for n in (0, 1, 2):
        loads[n].wait()
    for j in range(8):
        wst[j, :, :QC] = qw[:, j * QC : (j + 1) * QC].astype(jnp.bfloat16)
        wst[j, :, QC : QC + HEAD_DIM] = kw[:, j * HEAD_DIM : (j + 1) * HEAD_DIM].astype(
            jnp.bfloat16
        )
        wst[j, :, QC + HEAD_DIM :] = vw[:, j * HEAD_DIM : (j + 1) * HEAD_DIM].astype(jnp.bfloat16)
    wg[y, t] = wst[t]
    pl.semaphore_wait(barrier, len(greeted))

    pieces = [(0, 1), (1, 0), (3, 0), (1, 1), (3, 1), (2, 0), (2, 1)]
    for j, i in pieces:
        to = ((zh + j) % 4) * 2 + (c + i) % 2
        send(wst.at[to], wg.at[y, t], "b1", ("b1", j, i), dp, to)

    loads[3].wait()
    loads[4].wait()

    def norm_rows(n, carry):
        rows = pl.ds(pl.multiple_of(n * 16, 16), 16)
        values = hidden[rows, :].astype(jnp.float32)
        mean_square = jnp.mean(values * values, axis=-1, keepdims=True)
        normal = (values * lax.rsqrt(mean_square + epsilon) * gain[...]).astype(jnp.bfloat16)
        for m in range(8):
            xn[m, rows, :] = normal[:, m * K : (m + 1) * K]
        return carry

    lax.fori_loop(0, ROWS // 16, norm_rows, 0)

    mine = pl.ds(pl.multiple_of(c * HALF, HALF), HALF)
    for dz, i in PEERS:
        to = member(dz, i)
        send(xn.at[to, mine], a.at[k, mine], "a", ("a", dz, i), to * 4 + y, shifted(dz))
    a[k] = xn[k]

    arrival = [(0, 0)] + pieces
    for n, (j, i) in enumerate(arrival):
        at = wg.at[y, ((zh - j + 4) % 4) * 2 + (c + i) % 2]
        if n:
            received(("b1", j, i), at)
        if n % 2:
            send(at, at, "b", "b2", along_y(1), t)
            send(at, at, "b", ("b2", n), along_y(3), t)
        else:
            send(at, at, "b", ("b2", n), along_y(1), t)
            send(at, at, "b", "b2", along_y(3), t)

    loads[6].wait()
    og[zl, y] = ow[...].astype(jnp.bfloat16)
    at = og.at[zl, y]
    send(at, at, "o1", "o1", across, t)

    for n, (j, i) in enumerate(arrival):
        way = 1 + 2 * (n % 2)
        at = wg.at[(y + 4 - way) % 4, ((zh - j + 4) % 4) * 2 + (c + i) % 2]
        received(("b2", n), at)
        send(at, at, "b", "b3", along_y(way), t)

    loads[5].wait()
    diagonal = lax.broadcasted_iota(jnp.int32, (ROWS, ROWS), 0) == lax.broadcasted_iota(
        jnp.int32, (ROWS, ROWS), 1
    )
    lengths = jnp.sum(
        jnp.where(diagonal, len_row[...].astype(jnp.float32), 0.0), axis=-1, keepdims=True
    )
    lens[...] = lengths
    lane = lax.broadcasted_iota(jnp.int32, (1, HEAD_DIM), 1)
    index_row = (lane % 64).astype(jnp.float32)
    frequency = jnp.exp(-math.log(rope_base) * index_row / 64)
    angle = lengths * frequency
    cos[...] = jnp.cos(angle)
    sin[...] = jnp.where(lane < 64, -1.0, 1.0) * jnp.sin(angle)

    down = lax.broadcasted_iota(jnp.int32, (512, 512), 0)
    over = lax.broadcasted_iota(jnp.int32, (512, 512), 1)
    turn[...] = jnp.where(
        (down // 128 == (over // 32) % 4)
        & ((down // 32) % 4 == over // 128)
        & (down % 32 == over % 32),
        1.0,
        0.0,
    ).astype(jnp.bfloat16)

    for dz, i in [(1, 0), (0, 1), (0, 3), (1, 1), (1, 3), (0, 2), (1, 2)]:
        at = a.at[source(dz, i), mine]
        received(("a", dz, i), at)
        send(at, at, "a", "af", dp, mate)
    received("af", a.at[0:7, 0:HALF])
    received("b2", wg.at[0])

    units = [(0, 1), (0, 0), (1, 1), (1, 0)]

    def product(h, dz, i):
        part = (zl + dz) % 2
        at = (y + i) % 4
        rows = a[
            pl.ds(part * 4, 4),
            h * HALF : (h + 1) * HALF,
            pl.ds(pl.multiple_of(at * 256, 256), 256),
        ]
        return jnp.dot(
            rows.reshape(4 * HALF, 256),
            wg[at].reshape(256, WC),
            preferred_element_type=jnp.float32,
        )

    for h, dz in units:
        acc[h, dz] = product(h, dz, 0) + product(h, dz, 1) + product(h, dz, 3)
    received("b3", wg.at[0])

    upper_rows, lower_rows = slice(0, QUARTER), slice(QUARTER, HALF)

    def multiply(h, dz):
        pst[h, dz] = (
            (acc[h, dz] + product(h, dz, 2)).astype(jnp.bfloat16).reshape(4, HALF, WC)
        )

    def depart(h, dz):
        far = (x + 2) % 4
        send(pst.at[h, dz, far, upper_rows], cx.at[h, dz, 0], "c", ("far", h, dz, 0), along_x(1), t)
        send(pst.at[h, dz, far, lower_rows], cx.at[h, dz, 1], "c", ("far", h, dz, 1), along_x(3), t)
        send(
            pst.at[h, dz, (x + 1) % 4, lower_rows],
            cn.at[h, dz, 0, 1],
            "c",
            ("near", h, dz),
            along_x(1),
            t,
        )
        send(
            pst.at[h, dz, (x + 3) % 4, upper_rows],
            cn.at[h, dz, 1, 0],
            "c",
            ("near", h, dz),
            along_x(3),
            t,
        )

    def forward(h, dz):
        for side, rows in enumerate((upper_rows, lower_rows)):
            way = 1 + 2 * side
            received(("far", h, dz, side), cx.at[h, dz, side])
            cf[h, dz, side] = (
                cx[h, dz, side].astype(jnp.float32)
                + pst[h, dz, (x + way) % 4, rows].astype(jnp.float32)
            ).astype(jnp.bfloat16)
            send(
                cf.at[h, dz, side],
                cn.at[h, dz, side, side],
                "c",
                ("near", h, dz),
                along_x(way),
                t,
            )

    def summed(h, dz):
        received(("near", h, dz), cn.at[h, dz])
        return (
            pst[h, dz, x].astype(jnp.float32)
            + cn[h, dz, 0].reshape(HALF, WC).astype(jnp.float32)
            + cn[h, dz, 1].reshape(HALF, WC).astype(jnp.float32)
        )

    def cross(h):
        zst[h] = summed(h, 1).astype(jnp.bfloat16)
        send(zst.at[h], zrecv.at[h], "z", ("z", h), across, t)

    def collect(h):
        total = summed(h, 0)
        received(("z", h), zrecv.at[h])
        own[h * HALF : (h + 1) * HALF, :] = total + zrecv[h].astype(jnp.float32)

    multiply(0, 1)
    depart(0, 1)
    multiply(0, 0)
    depart(0, 0)
    multiply(1, 1)
    forward(0, 1)
    depart(1, 1)
    multiply(1, 0)
    forward(0, 0)
    depart(1, 0)
    at = og.at[zl, y]
    for i in (2, 1, 3):
        send(at, at, "o2", "o2", along_y(i), t)
    at = og.at[1 - zl, y]
    received("o1", at)
    for i in (2, 1, 3):
        send(at, at, "o2", "o2", along_y(i), t)
    for n in (7, 8, 9):
        loads[n].wait()

    scale = 1.0 / math.sqrt(HEAD_DIM)
    wide = BLOCK_ROWS * CACHE
    tall = BLOCK_ROWS * GROUP
    row_of = lax.broadcasted_iota(jnp.int32, (tall, wide), 0) % BLOCK_ROWS
    column = lax.broadcasted_iota(jnp.int32, (tall, wide), 1)
    same = row_of == column // CACHE
    position = (column % CACHE).astype(jnp.float32)

    def attend(h):
        chunk = slice(h * CR, (h + 1) * CR)
        cosine = cos[chunk, :]
        sine = sin[chunk, :]
        for m in range(GROUP + 1):
            columns = slice(m * HEAD_DIM, (m + 1) * HEAD_DIM)
            head = own[chunk, columns]
            head = head * cosine + pltpu.roll(head, 64, 1) * sine
            own[chunk, columns] = head.astype(jnp.bfloat16).astype(jnp.float32)
        fresh_v[chunk, :] = own[chunk, QC : QC + HEAD_DIM].astype(jnp.bfloat16)
        value_b = own[chunk, QC + HEAD_DIM :].astype(jnp.bfloat16)
        value_v[chunk, :] = value_b
        own[chunk, QC + HEAD_DIM :] = value_b.astype(jnp.float32)
        for n in range(h * CR // BLOCK_ROWS, (h + 1) * CR // BLOCK_ROWS):
            rows = slice(n * BLOCK_ROWS, (n + 1) * BLOCK_ROWS)
            query = jnp.concatenate(
                [own[rows, m * HEAD_DIM : (m + 1) * HEAD_DIM] for m in range(GROUP)], axis=0
            )
            fresh = jnp.concatenate([own[rows, QC : QC + HEAD_DIM]] * GROUP, axis=0)
            length = jnp.concatenate([lens[rows, :]] * GROUP, axis=0)
            scores = (
                lax.dot_general(
                    query.astype(jnp.bfloat16),
                    kc[n * wide : (n + 1) * wide, :],
                    (((1,), (1,)), ((), ())),
                    preferred_element_type=jnp.float32,
                )
                * scale
            )
            self_score = jnp.sum(query * fresh, axis=-1, keepdims=True) * scale
            kept = same & (position < length)
            scores = jnp.where(kept, scores, -jnp.inf)
            largest = jnp.maximum(jnp.max(scores, axis=-1, keepdims=True), self_score)
            kept_exp = jnp.exp(scores - largest)
            own_exp = jnp.exp(self_score - largest)
            divisor = jnp.sum(kept_exp, axis=-1, keepdims=True) + own_exp
            probs[n] = (kept_exp / divisor).astype(jnp.bfloat16)
            own_prob = (own_exp / divisor).astype(jnp.bfloat16).astype(jnp.float32)
            value = jnp.concatenate([own[rows, QC + HEAD_DIM :]] * GROUP, axis=0)
            attended = (
                jnp.dot(
                    probs[n],
                    vc[n * wide : (n + 1) * wide, :],
                    preferred_element_type=jnp.float32,
                )
                + own_prob * value
            )
            for m in range(GROUP):
                att32[rows, m * HEAD_DIM : (m + 1) * HEAD_DIM] = attended[
                    m * BLOCK_ROWS : (m + 1) * BLOCK_ROWS
                ]
        attg[h, t, x] = att32[chunk, :].astype(jnp.bfloat16)
        at = attg.at[h, t, x]
        send(at, at, ("z", h), ("z1", h, 1), dp, along_z(1))
        send(at, at, ("z", h), ("z1", h, 3), dp, along_z(3))
        spread_x(h, 0)

    def tq(d):
        return ((zh + d) % 4) * 2 + c

    def xq(i):
        return (x + i) % 4

    lower, upper = slice(0, CH), slice(CH, CR)

    def hand(n, at):
        send(at, at, ("x", n), ("hand", n), dp, mate)

    def spread_x(n, d):
        at = attg.at[n, tq(d), x]
        send(at, at, ("x", n), ("x1", n, d, 1), along_x(1), t)
        send(at, at, ("x", n), ("x1", n, d, 3), along_x(3), t)
        hand(n, at)

    def z_first(n):
        received(("z1", n, 1), attg.at[n, tq(3), x])
        at = attg.at[n, tq(3), x, lower]
        send(at, at, ("z", n), ("z2", n), dp, along_z(1))
        received(("z1", n, 3), attg.at[n, tq(1), x])
        at = attg.at[n, tq(1), x, upper]
        send(at, at, ("z", n), ("z2", n), dp, along_z(3))
        spread_x(n, 3)
        spread_x(n, 1)

    def z_second(n):
        received(("z2", n), attg.at[n, tq(2), x])
        spread_x(n, 2)

    def x_first(n):
        for d in (0, 3, 1, 2):
            at = attg.at[n, tq(d), xq(3)]
            received(("x1", n, d, 1), at)
            send(at.at[lower], at.at[lower], ("x", n), ("x2", n), along_x(1), t)
            hand(n, at)
            at = attg.at[n, tq(d), xq(1)]
            received(("x1", n, d, 3), at)
            send(at.at[upper], at.at[upper], ("x", n), ("x2", n), along_x(3), t)
            hand(n, at)

    def x_second(n):
        received(("x2", n), attg.at[n, 0])
        for d in (0, 3, 1, 2):
            hand(n, attg.at[n, tq(d), xq(2)])

    def project(n):
        received(("hand", n), attg.at[n, 0:4])
        out = jnp.zeros((4 * CR, FEATURES), jnp.float32)
        for j in range(8):
            out += lax.dot_general(
                attg[n, j].reshape(4 * CR, QC),
                og[:, :, :, j * QC : (j + 1) * QC].reshape(FEATURES, QC),
                (((1,), (1,)), ((), ())),
                preferred_element_type=jnp.float32,
            )
        made[n] = out.astype(jnp.bfloat16).reshape(4, CR, FEATURES)
        for i in (2, 1, 3):
            send(made.at[n, xq(i)], gall.at[n, t, x], ("t", n), ("t", n), along_x(i), t)
        gall[n, t, x] = made[n, x]

    def gather_first(n):
        received(("t", n), made.at[n, 0:3])
        at = gall.at[n, t]
        send(at, at, ("u", n), ("u1", n, 1), dp, along_z(1))
        send(at, at, ("u", n), ("u1", n, 3), dp, along_z(3))
        send(at, at, ("u", n), ("last", n), dp, mate)

    def gather_second(n):
        for way in (1, 3):
            at = gall.at[n, tq(4 - way)]
            received(("u1", n, way), at)
            part = at.at[pl.ds(way - 1, 2)]
            send(part, part, ("u", n), ("u2", n), dp, along_z(way))
            send(at, at, ("u", n), ("last", n), dp, mate)

    def gather_third(n):
        at = gall.at[n, tq(2)]
        received(("u2", n), at)
        send(at, at, ("u", n), ("last", n), dp, mate)

    stores = []

    def store(src, dst):
        copy = pltpu.make_async_copy(src, dst, out_sem.at[len(stores)])
        copy.start()
        stores.append(copy)

    def finish(n):
        received(("last", n), gall.at[n, 0:4])
        for part in range(16):
            i, q, r = part // 4, (part // 2) % 2, part % 2
            for s in range(4):
                runs[part, :, s * 128 : (s + 1) * 128] = gall[
                    n, 4 * q + s, i, :, r * 128 : (r + 1) * 128
                ]
        ordered[...] = jnp.dot(
            runs[...].reshape(16 * CR, 512), turn[...], preferred_element_type=jnp.float32
        ).reshape(16, CR, 512)
        for m in range(CR // 16):
            rows = slice(n * CR + m * 16, n * CR + (m + 1) * 16)
            squares = jnp.zeros((16, 128), jnp.float32)
            for part in range(16):
                i, q, r = part // 4, (part // 2) % 2, part % 2
                for s in range(4):
                    at = (r * 16 + i * 4 + s) * 256 + q * 128
                    columns = slice(at, at + 128)
                    value = (
                        hidden[rows, columns].astype(jnp.float32)
                        + ordered[part, m * 16 : (m + 1) * 16, s * 128 : (s + 1) * 128]
                    )
                    new_v[rows, columns] = value.astype(jnp.bfloat16)
                    residual[:, columns] = value
                    squares += value * value
            mean_square = jnp.sum(squares, axis=-1, keepdims=True) * (1.0 / D)
            factor = lax.rsqrt(mean_square + epsilon)
            normed_v[rows, :] = (residual[...] * factor * post[...]).astype(jnp.bfloat16)
        rows = pl.ds(n * CR, CR)
        store(new_v.at[rows], new_out.at[rows])
        store(normed_v.at[rows], normed_out.at[rows])

    steps = []

    def at_time(when, name, act, *args):
        steps.append((when, len(steps), name, act, args))

    at_time(1.0, "cross0", cross, 0)
    at_time(2.0, "forward11", forward, 1, 1)
    at_time(3.0, "collect0", collect, 0)
    at_time(4.0, "att0", attend, 0)
    at_time(5.0, "att1", attend, 1)
    at_time(5.1, "forward10", forward, 1, 0)
    at_time(6.0, "cross1", cross, 1)
    at_time(7.5, "collect1", collect, 1)
    at_time(9.0, "att2", attend, 2)
    at_time(10.4, "att3", attend, 3)
    for n, when in enumerate((9.5, 11.0, 14.5, 16.0)):
        at_time(when, f"z_first{n}", z_first, n)
        at_time(when + 3.0, f"z_second{n}", z_second, n)
    for n, when in enumerate((15.0, 17.5, 21.0, 24.0)):
        at_time(when, f"x_first{n}", x_first, n)
        at_time(when + 3.2, f"x_second{n}", x_second, n)
    for n, when in enumerate((19.5, 22.5, 26.0, 30.0)):
        at_time(when, f"project{n}", project, n)
        at_time(when + 4.0, f"gather_first{n}", gather_first, n)
    for n, when in enumerate((28.0, 32.5, 37.0, 41.5)):
        at_time(when, f"gather_second{n}", gather_second, n)
        at_time(when + 3.0, f"gather_third{n}", gather_third, n)
        at_time(when + 5.0, f"finish{n}", finish, n)
    waited = False
    for when, _, name, act, args in sorted(steps, key=lambda step: step[:2]):
        if act is project and not waited:
            received("o2", og.at[:, 0:3])
            waited = True
        act(*args)

    store(fresh_v, fresh_out)
    store(value_v, value_out)
    departed("b1", wst.at[0:7])
    departed("a", a.at[0:7])
    departed("b", wg.at[0:3])
    departed("c", pst.at[:, :, 0:3])
    departed("z", zst)
    departed("o1", og.at[0, 0])
    departed("o2", og.at[:, 0:3])
    for n in range(CHUNKS):
        departed(("x", n), attg.at[n, 0:7])
        departed(("z", n), attg.at[n, 0, 0:3])
        departed(("t", n), made.at[n, 0:3])
        departed(("u", n), gall.at[n, 0:7])
    assert not in_size and not out_size
    for copy in stores:
        copy.wait()


def copy_out(a_in, b_in, c_in, d_in, a_out, b_out, c_out, d_out, a, b, c, d, sem):
    parts = 4
    rows = ROWS // parts
    ins, outs = [], []
    for src, hold, dst in ((a_in, a, a_out), (b_in, b, b_out)):
        for n in range(parts):
            at = pl.ds(n * rows, rows)
            ins.append((src.at[at], hold.at[at]))
            outs.append((hold.at[at], dst.at[at]))
    ins += [(c_in, c), (d_in, d)]
    outs += [(c, c_out), (d, d_out)]
    first = [pltpu.make_async_copy(s, h, sem.at[0, n]) for n, (s, h) in enumerate(ins)]
    second = [pltpu.make_async_copy(h, s, sem.at[1, n]) for n, (h, s) in enumerate(outs)]
    for copy in first:
        copy.start()
    for before, after in zip(first, second):
        before.wait()
        after.start()
    for copy in second:
        copy.wait()


def shards(
    hidden,
    q_weight,
    k_weight,
    v_weight,
    o_weight,
    input_gain,
    post_gain,
    key_cache,
    value_cache,
    lengths,
):
    kc = jnp.transpose(key_cache, (0, 2, 1, 3)).reshape(ROWS * CACHE, HEAD_DIM)
    vc = jnp.transpose(value_cache, (0, 2, 1, 3)).reshape(ROWS * CACHE, HEAD_DIM)
    bf16, f32 = jnp.bfloat16, jnp.float32
    dma = pltpu.SemaphoreType.DMA
    results = (
        jax.ShapeDtypeStruct((ROWS, D), bf16),
        jax.ShapeDtypeStruct((ROWS, D), bf16),
        jax.ShapeDtypeStruct((ROWS, HEAD_DIM), bf16),
        jax.ShapeDtypeStruct((ROWS, HEAD_DIM), bf16),
    )
    held = pl.pallas_call(
        kernel,
        out_shape=results,
        in_specs=[pl.BlockSpec(memory_space=pl.ANY)] * 10,
        out_specs=[pl.BlockSpec(memory_space=pl.ANY)] * 4,
        scratch_shapes=[
            pltpu.VMEM((ROWS, D), bf16),
            pltpu.VMEM((32, QD), f32),
            pltpu.VMEM((32, 1024), f32),
            pltpu.VMEM((32, 1024), f32),
            pltpu.VMEM((32, QD), f32),
            pltpu.VMEM((1, D), f32),
            pltpu.VMEM((1, D), f32),
            pltpu.VMEM((ROWS * CACHE, HEAD_DIM), bf16),
            pltpu.VMEM((ROWS * CACHE, HEAD_DIM), bf16),
            pltpu.VMEM((1, ROWS), jnp.int32),
            pltpu.VMEM((ROWS, 1), f32),
            pltpu.VMEM((ROWS, HEAD_DIM), f32),
            pltpu.VMEM((ROWS, HEAD_DIM), f32),
            pltpu.VMEM((8, ROWS, K), bf16),
            pltpu.VMEM((8, 32, WC), bf16),
            pltpu.VMEM((4, 8, 32, WC), bf16),
            pltpu.VMEM((2, 4, 32, QD), bf16),
            pltpu.VMEM((8, ROWS, K), bf16),
            pltpu.VMEM((2, 2, 4 * HALF, WC), f32),
            pltpu.VMEM((2, 2, 4, HALF, WC), bf16),
            pltpu.VMEM((2, 2, 2, QUARTER, WC), bf16),
            pltpu.VMEM((2, 2, 2, 2, QUARTER, WC), bf16),
            pltpu.VMEM((2, 2, 2, QUARTER, WC), bf16),
            pltpu.VMEM((2, HALF, WC), bf16),
            pltpu.VMEM((2, HALF, WC), bf16),
            pltpu.VMEM((ROWS, WC), f32),
            pltpu.VMEM((ROWS // BLOCK_ROWS, BLOCK_ROWS * GROUP, BLOCK_ROWS * CACHE), bf16),
            pltpu.VMEM((ROWS, QC), f32),
            pltpu.VMEM((CHUNKS, 8, 4, CR, QC), bf16),
            pltpu.VMEM((CHUNKS, 4, CR, FEATURES), bf16),
            pltpu.VMEM((CHUNKS, 8, 4, CR, FEATURES), bf16),
            pltpu.VMEM((512, 512), bf16),
            pltpu.VMEM((16, CR, 512), bf16),
            pltpu.VMEM((16, CR, 512), f32),
            pltpu.VMEM((16, D), f32),
            pltpu.VMEM((ROWS, D), bf16),
            pltpu.VMEM((ROWS, D), bf16),
            pltpu.VMEM((ROWS, HEAD_DIM), bf16),
            pltpu.VMEM((ROWS, HEAD_DIM), bf16),
            dma((10,)),
            dma((2 * CHUNKS + 2,)),
            dma((SENDS,)),
            dma((RECEIVES,)),
        ],
        compiler_params=pltpu.CompilerParams(collective_id=0, has_side_effects=True),
    )(
        hidden,
        q_weight,
        k_weight,
        v_weight,
        o_weight,
        input_gain.reshape(1, D),
        post_gain.reshape(1, D),
        kc,
        vc,
        lengths.reshape(1, ROWS),
    )
    new_hidden, normed, fresh, values = pl.pallas_call(
        copy_out,
        out_shape=results,
        in_specs=[pl.BlockSpec(memory_space=pl.ANY)] * 4,
        out_specs=[pl.BlockSpec(memory_space=pl.ANY)] * 4,
        scratch_shapes=[
            pltpu.VMEM((ROWS, D), bf16),
            pltpu.VMEM((ROWS, D), bf16),
            pltpu.VMEM((ROWS, HEAD_DIM), bf16),
            pltpu.VMEM((ROWS, HEAD_DIM), bf16),
            dma((2, 10)),
        ],
    )(*held)
    return (
        new_hidden,
        normed,
        fresh.reshape(ROWS, 1, HEAD_DIM),
        values.reshape(ROWS, 1, HEAD_DIM),
    )


def solution(mesh):
    in_specs = (
        P("dp", None),
        P(("dp", "tensor"), None),
        P(("dp", "tensor"), None),
        P(("dp", "tensor"), None),
        P(("dp", "tensor"), None),
        P(),
        P(),
        P("dp", None, "tensor", None),
        P("dp", None, "tensor", None),
        P("dp"),
    )
    out_specs = (P("dp", None), P("dp", None), P("dp", "tensor", None), P("dp", "tensor", None))
    return jax.shard_map(shards, mesh=mesh, in_specs=in_specs, out_specs=out_specs, check_vma=False)
```
